32 devices in a mesh: dp: 4 (over x, core), tm: 2 (over y), height: 4 (over z).
Axes of the slice: x: 2, y: 2, z: 4, core: 2. Of those that a mesh axis runs over, the one named last changes fastest.
Arguments:
- latent: bfloat16 [16, 8, 16, 512], P(('dp', 'tm'), None, None, 'height'), parts along dimension 0, may hold values from -6 to 6
- gain_latent: float32 [512], P('height'), may hold values from 0.25 to 1.75
- shift_latent: float32 [512], P('height'), may hold values from -3 to 3
- conv_latent: bfloat16 [13824, 512], P('tm', 'height'), may hold values from -0.0546875 to 0.0546875
- up_weight: bfloat16 [512, 2048], P('height'), may hold values from -0.25 to 0.25
- gain_block: float32 [256], replicated, may hold values from 0.25 to 1.75
- shift_block: float32 [256], replicated, may hold values from -3 to 3
- conv_block: bfloat16 [6912, 256], P(('tm', 'height')), may hold values from -0.078125 to 0.078125
- cotangent: bfloat16 [32, 16, 32, 256], P(('dp', 'tm'), 'height'), parts along dimension 0, may hold values from -6 to 6
Outputs:
- decoded: bfloat16 [32, 16, 32, 256], P(('dp', 'tm'), 'height'), parts along dimension 0
- grad_upsampled: bfloat16 [32, 16, 32, 256], P(('dp', 'tm'), 'height'), parts along dimension 0
- grad_weight: float32 [9216, 256], P(('dp', 'tm', 'height')), parts along dimension 0
- grad_gain: float32 [1024], P('dp'), parts along dimension 0
- grad_shift: float32 [1024], P('dp'), parts along dimension 0
The draws below stay inside these ranges and needn't reach their ends.
There are 4 independent parts, one for each index of `dp`. The reference program is written for one: setup_inputs(seed, part) draws one part's arguments, and reference() takes and returns one part's arrays. A program takes and returns all parts, laid end to end along the dimension named above; an argument that names none is the same for every part. Nothing has to cross between parts.
All inputs are finite; a program needn't handle non-finite values.
Results may differ from the reference program's by a relative error of at most 0.009.
Values may be sent and summed in bfloat16 or wider, within the bound.
A program may use at most 128 MiB of HBM per device.

```python
import jax
import jax.numpy as jnp
from jax import lax

C1 = 512
C2 = 256
GROUPS = 32
W1 = 16
H1 = 8
FRAMES = 4
FRAMES_UP = 8
ROWS_UP = 16
COLS_UP = 32
N_TM = 2
N_HEIGHT = 4


def level_of(rng, shape, pieces, least, high):
    gain = 1.0
    for position, shards_of in pieces:
        steps = jax.random.uniform(jax.random.fold_in(jax.random.fold_in(rng, 6), position), (shards_of,), jnp.float32, least / len(pieces), high / len(pieces))
        gain = gain * jnp.repeat(jnp.exp(steps), shape[position] // shards_of).reshape((-1,) + (1,) * (len(shape) - 1 - position))
    return gain


def noise(own_key, shape, scale, bound, split=(), kind=jnp.bfloat16):
    array = scale * jax.random.normal(own_key, shape, jnp.float32)
    if split:
        array = array * level_of(own_key, shape, split, -0.22, 0.18)
    return jnp.clip(array, -bound, bound).astype(kind)


def setup_inputs(seed: int = 0, part: int = 0) -> dict:
    streams_of = jax.random.split(jax.random.key(seed), 10)
    part_keys = jax.random.split(jax.random.fold_in(streams_of[9], part), 10)
    return {
        "latent": noise(part_keys[0], (FRAMES, H1, W1, C1), 1.0, 6.0, ((0, 2), (3, 4))),
        "gain_latent": jnp.clip(1.0 + 0.15 * jax.random.normal(streams_of[1], (C1,), jnp.float32), 0.25, 1.75),
        "shift_latent": noise(streams_of[2], (C1,), 0.5, 3.0, ((0, 4),), jnp.float32),
        "conv_latent": noise(streams_of[3], (27 * C1, C1), (27 * C1) ** -0.5, 0.0546875, ((0, 2), (1, 4))),
        "up_weight": noise(streams_of[4], (C1, 8 * C2), C1 ** -0.5, 0.25, ((0, 4),)),
        "gain_block": jnp.clip(1.0 + 0.15 * jax.random.normal(streams_of[5], (C2,), jnp.float32), 0.25, 1.75),
        "shift_block": noise(streams_of[6], (C2,), 0.5, 3.0, (), jnp.float32),
        "conv_block": noise(streams_of[7], (27 * C2, C2), (27 * C2) ** -0.5, 0.078125, ((0, 8),)),
        "cotangent": noise(part_keys[8], (FRAMES_UP, ROWS_UP, COLS_UP, C2), 1.0, 6.0, ((0, 2), (1, 4))),
    }


epsilon = 1e-06

def moments(values, groups):
    grouped = values.reshape(-1, groups, values.shape[-1] // groups)
    count_cells = grouped.shape[0] * grouped.shape[2]
    mean_value = lax.optimization_barrier(jnp.sum(grouped, axis=(0, 2))) / count_cells
    mean_square = lax.optimization_barrier(jnp.sum(grouped * grouped, axis=(0, 2))) / count_cells
    inverse = lax.rsqrt(mean_square - mean_value * mean_value + epsilon)
    return (mean_value, inverse)

def standardize(values, mean_value, inverse, groups):
    shape_full = values.shape
    grouped = values.reshape(shape_full[:-1] + (groups, shape_full[-1] // groups))
    return ((grouped - mean_value[:, None]) * inverse[:, None]).reshape(shape_full)

def causal_taps(padded, weight, frames, rows, cols):
    channels_in = padded.shape[-1]
    summed = jnp.zeros((frames * rows * cols, weight.shape[1]), jnp.float32)
    for lag_step in range(3):
        for row_step in range(3):
            for col_step in range(3):
                tap_index = (lag_step * 3 + row_step) * 3 + col_step
                window = padded[lag_step:lag_step + frames, row_step:row_step + rows, col_step:col_step + cols]
                kernel = weight[tap_index * channels_in:(tap_index + 1) * channels_in]
                summed = summed + jnp.dot(window.reshape(-1, channels_in), kernel, preferred_element_type=jnp.float32)
    return summed.reshape(frames, rows, cols, weight.shape[1])

def transposed_taps(padded, weight, frames, rows, cols):
    channels_out = padded.shape[-1]
    channels_in = weight.shape[0] // 27
    summed = jnp.zeros((frames * rows * cols, channels_in), jnp.float32)
    for lag_step in range(3):
        for row_step in range(3):
            for col_step in range(3):
                tap_index = (lag_step * 3 + row_step) * 3 + col_step
                window = padded[2 - lag_step:2 - lag_step + frames, 2 - row_step:2 - row_step + rows, 2 - col_step:2 - col_step + cols]
                kernel = weight[tap_index * channels_in:(tap_index + 1) * channels_in]
                summed = summed + lax.dot_general(window.reshape(-1, channels_out), kernel, (((1,), (1,)), ((), ())), preferred_element_type=jnp.float32)
    return summed.reshape(frames, rows, cols, channels_in)

def weight_terms(padded, grads, frames, rows, cols):
    channels_in = padded.shape[-1]
    flat_grads = grads.reshape(-1, grads.shape[-1])
    blocks = []
    for row_step in range(3):
        for col_step in range(3):
            window = padded[2:2 + frames, row_step:row_step + rows, col_step:col_step + cols]
            blocks.append(lax.dot_general(window.reshape(-1, channels_in), flat_grads, (((0,), (0,)), ((), ())), preferred_element_type=jnp.float32))
    return jnp.concatenate(blocks, 0)

def reference(latent, gain_latent, shift_latent, conv_latent, up_weight, gain_block, shift_block, conv_block, cotangent):
    latent_f32 = latent.astype(jnp.float32)
    mean_latent, inverse_latent = moments(latent_f32, GROUPS)
    normed = standardize(latent_f32, mean_latent, inverse_latent, GROUPS) * gain_latent + shift_latent
    active = jax.nn.silu(normed).astype(jnp.bfloat16)
    frames_latent, rows_latent, cols_latent = (latent.shape[0], latent.shape[1], latent.shape[2])
    padded = jnp.pad(active, ((2, 0), (1, 1), (1, 1), (0, 0)))
    mixed = causal_taps(padded, conv_latent, frames_latent, rows_latent, cols_latent)
    refined = (latent_f32 + mixed).astype(jnp.bfloat16)
    expanded = jnp.dot(refined.reshape(-1, C1), up_weight, preferred_element_type=jnp.float32)
    spread = expanded.reshape(frames_latent, rows_latent, cols_latent, 2, 2, 2, C2)
    spread = spread.transpose(0, 3, 1, 4, 2, 5, 6)
    upsampled = spread.reshape(2 * frames_latent, 2 * rows_latent, 2 * cols_latent, C2).astype(jnp.bfloat16)
    frames_block, rows_block, cols_block = (upsampled.shape[0], upsampled.shape[1], upsampled.shape[2])
    up_f32 = upsampled.astype(jnp.float32)
    mean_block, inverse_block = moments(up_f32, GROUPS)
    standard = standardize(up_f32, mean_block, inverse_block, GROUPS)
    normed_block = standard * gain_block + shift_block
    active_block = jax.nn.silu(normed_block).astype(jnp.bfloat16)
    padded_block = jnp.pad(active_block, ((2, 0), (1, 1), (1, 1), (0, 0)))
    mixed_block = causal_taps(padded_block, conv_block, frames_block, rows_block, cols_block)
    decoded = (up_f32 + mixed_block).astype(jnp.bfloat16)
    grad_padded = jnp.pad(cotangent, ((0, 2), (1, 1), (1, 1), (0, 0)))
    grad_active = transposed_taps(grad_padded, conv_block, frames_block, rows_block, cols_block)
    frames_dev = frames_block // N_TM
    rows_dev = rows_block // N_HEIGHT
    zero_index = jnp.zeros((), jnp.int32)

    def add_device(carried, device):
        time_start = device // N_HEIGHT * frames_dev
        row_start = device % N_HEIGHT * rows_dev
        region = lax.dynamic_slice(padded_block, (time_start, row_start, zero_index, zero_index), (frames_dev + 2, rows_dev + 2, cols_block + 2, C2))
        grads = lax.dynamic_slice(cotangent, (time_start, row_start, zero_index, zero_index), (frames_dev, rows_dev, cols_block, C2))
        term = weight_terms(region, grads, frames_dev, rows_dev, cols_block)
        return (carried + term, None)
    grad_weight, unused = lax.scan(add_device, jnp.zeros((9 * C2, C2), jnp.float32), jnp.arange(N_TM * N_HEIGHT, dtype=jnp.int32))
    sigmoid = jax.nn.sigmoid(normed_block)
    grad_normed = grad_active * sigmoid * (1.0 + normed_block * (1.0 - sigmoid))
    flat_grad = grad_normed.reshape(-1, C2)
    flat_standard = standard.reshape(-1, C2)
    grad_shift = lax.optimization_barrier(jnp.sum(flat_grad, axis=0))
    grad_gain = lax.optimization_barrier(jnp.sum(flat_grad * flat_standard, axis=0))
    per_block = C2 // GROUPS
    count_block = flat_grad.shape[0] * per_block
    first_mean = lax.optimization_barrier(jnp.sum((gain_block * grad_shift).reshape(GROUPS, per_block), axis=1)) / count_block
    second_mean = lax.optimization_barrier(jnp.sum((gain_block * grad_gain).reshape(GROUPS, per_block), axis=1)) / count_block
    grouped_grad = (grad_normed * gain_block).reshape(-1, GROUPS, per_block)
    grouped_standard = standard.reshape(-1, GROUPS, per_block)
    corrected = (grouped_grad - first_mean[:, None] - grouped_standard * second_mean[:, None]) * inverse_block[:, None]
    grad_upsampled = (cotangent.astype(jnp.float32) + corrected.reshape(cotangent.shape)).astype(jnp.bfloat16)
    return (decoded, grad_upsampled, grad_weight, grad_gain, grad_shift)
```

```python
import functools

import jax
import jax.numpy as jnp
from jax import lax
from jax.experimental import pallas as pl
from jax.experimental.pallas import tpu as pltpu
from jax.sharding import PartitionSpec as P

C1 = 512
GROUPS = 32


epsilon = 1e-06


def shifted(block, axis, distance):
    devices = range(lax.axis_size(axis))
    route = [(i - distance, i) for i in devices if i - distance in devices]
    return lax.ppermute(block, axis, route)


def extended_2(cells, sides, width):
    for axis, dim in sides:
        count = lax.axis_size(axis)
        ends = count - 1
        head = lax.slice_in_dim(cells, 0, width, axis=dim)
        tail = lax.slice_in_dim(cells, cells.shape[dim] - width, cells.shape[dim], axis=dim)
        cells = jnp.concatenate(
            [
                lax.ppermute(tail, axis, [(i, (i + 1) % count) for i in range(ends)]),
                cells,
                lax.ppermute(head, axis, [((i + 1) % count, i) for i in range(ends)]),
            ],
            axis=dim,
        )
    return cells


def standardize(values, mean_value, inverse, groups):
    shape_full = values.shape
    grouped = values.reshape(shape_full[:-1] + (groups, shape_full[-1] // groups))
    return ((grouped - mean_value[:, None]) * inverse[:, None]).reshape(shape_full)


def causal_taps(padded, weight, frames, rows, cols):
    channels_in = padded.shape[-1]
    summed = jnp.zeros((frames * rows * cols, weight.shape[1]), jnp.float32)
    for lag_step in range(3):
        for row_step in range(3):
            for col_step in range(3):
                tap_index = (lag_step * 3 + row_step) * 3 + col_step
                window = padded[
                    lag_step : lag_step + frames,
                    row_step : row_step + rows,
                    col_step : col_step + cols,
                ]
                kernel = weight[tap_index * channels_in : (tap_index + 1) * channels_in]
                summed = summed + jnp.dot(
                    window.reshape(-1, channels_in), kernel, preferred_element_type=jnp.float32
                )
    return summed.reshape(frames, rows, cols, weight.shape[1])


def transposed_taps(padded, weight, frames, rows, cols):
    channels_out = padded.shape[-1]
    channels_in = weight.shape[0] // 27
    summed = jnp.zeros((frames * rows * cols, channels_in), jnp.float32)
    for lag_step in range(3):
        for row_step in range(3):
            for col_step in range(3):
                tap_index = (lag_step * 3 + row_step) * 3 + col_step
                window = padded[
                    2 - lag_step : 2 - lag_step + frames,
                    2 - row_step : 2 - row_step + rows,
                    2 - col_step : 2 - col_step + cols,
                ]
                kernel = weight[tap_index * channels_in : (tap_index + 1) * channels_in]
                summed = summed + lax.dot_general(
                    window.reshape(-1, channels_out),
                    kernel,
                    (((1,), (1,)), ((), ())),
                    preferred_element_type=jnp.float32,
                )
    return summed.reshape(frames, rows, cols, channels_in)


def weight_terms(padded, grads, frames, rows, cols):
    channels_in = padded.shape[-1]
    flat_grads = grads.reshape(-1, grads.shape[-1])
    blocks = []
    for row_step in range(3):
        for col_step in range(3):
            window = padded[2 : 2 + frames, row_step : row_step + rows, col_step : col_step + cols]
            blocks.append(
                lax.dot_general(
                    window.reshape(-1, channels_in),
                    flat_grads,
                    (((0,), (0,)), ((), ())),
                    preferred_element_type=jnp.float32,
                )
            )
    return jnp.concatenate(blocks, 0)


def local(
    latent,
    gain_latent,
    shift_latent,
    conv_latent,
    up_weight,
    gain_block,
    shift_block,
    conv_block,
    cotangent,
):
    per_group = C1 // GROUPS
    groups_here = latent.shape[-1] // per_group
    latent_f32 = latent.astype(jnp.float32)
    grouped = latent_f32.reshape(-1, groups_here, per_group)
    first_sums = jnp.sum(grouped, axis=(0, 2))
    second_sums = jnp.sum(grouped * grouped, axis=(0, 2))
    first_totals, second_totals = lax.psum((first_sums, second_sums), "tm")
    count_latent = grouped.shape[0] * per_group * lax.axis_size("tm")
    mean_latent = first_totals / count_latent
    inverse_latent = lax.rsqrt(second_totals / count_latent - mean_latent * mean_latent + epsilon)
    normed = (
        standardize(latent_f32, mean_latent, inverse_latent, groups_here) * gain_latent
        + shift_latent
    )
    active = jax.nn.silu(normed).astype(jnp.bfloat16)
    earlier = shifted(active, "tm", 1)
    extended = jnp.concatenate([earlier, active], 0)
    all_channels = lax.all_gather(extended, "height", axis=3, tiled=True)
    padded = jnp.pad(all_channels, ((0, 0), (1, 1), (1, 1), (0, 0)))
    latent_weight = lax.all_gather(conv_latent, "tm", axis=0, tiled=True)
    frames_latent, rows_latent, cols_latent = (latent.shape[0], latent.shape[1], latent.shape[2])
    mixed = causal_taps(padded, latent_weight, frames_latent, rows_latent, cols_latent)
    refined = (latent_f32 + mixed).astype(jnp.bfloat16)
    band_rows = rows_latent // lax.axis_size("height")
    own_band = lax.all_to_all(refined, "height", split_axis=1, concat_axis=3, tiled=True)
    flat_band = own_band.reshape(-1, own_band.shape[-1])
    expanded = jnp.dot(
        flat_band,
        lax.all_gather(up_weight, "height", axis=0, tiled=True),
        preferred_element_type=jnp.float32,
    )
    channels_block = up_weight.shape[1] // 8
    spread = expanded.reshape(frames_latent, band_rows, cols_latent, 2, 2, 2, channels_block)
    spread = spread.transpose(0, 3, 1, 4, 2, 5, 6)
    upsampled = spread.reshape(
        2 * frames_latent, 2 * band_rows, 2 * cols_latent, channels_block
    ).astype(jnp.bfloat16)
    frames_block, rows_block, cols_block = (
        upsampled.shape[0],
        upsampled.shape[1],
        upsampled.shape[2],
    )
    up_f32 = upsampled.astype(jnp.float32)
    per_block = channels_block // GROUPS
    grouped_block = up_f32.reshape(-1, GROUPS, per_block)
    block_first = jnp.sum(grouped_block, axis=(0, 2))
    block_second = jnp.sum(grouped_block * grouped_block, axis=(0, 2))
    block_first, block_second = lax.psum((block_first, block_second), ("tm", "height"))
    count_block = grouped_block.shape[0] * per_block * lax.axis_size("tm") * lax.axis_size("height")
    mean_block = block_first / count_block
    inverse_block = lax.rsqrt(block_second / count_block - mean_block * mean_block + epsilon)
    standard = standardize(up_f32, mean_block, inverse_block, GROUPS)
    normed_block = standard * gain_block + shift_block
    active_block = jax.nn.silu(normed_block).astype(jnp.bfloat16)
    before = shifted(active_block[-2:], "tm", 1)
    ext_block = jnp.concatenate([before, active_block], 0)
    beside_all = extended_2(ext_block, (("height", 1),), 1)
    padded_block = jnp.pad(beside_all, ((0, 0), (0, 0), (1, 1), (0, 0)))
    block_weight = lax.all_gather(conv_block, ("tm", "height"), axis=0, tiled=True)
    mixed_block = causal_taps(padded_block, block_weight, frames_block, rows_block, cols_block)
    decoded = (up_f32 + mixed_block).astype(jnp.bfloat16)
    after = shifted(cotangent[:2], "tm", -1)
    grad_ext = jnp.concatenate([cotangent, after], 0)
    grad_around = extended_2(grad_ext, (("height", 1),), 1)
    grad_padded = jnp.pad(grad_around, ((0, 0), (0, 0), (1, 1), (0, 0)))
    grad_active = transposed_taps(grad_padded, block_weight, frames_block, rows_block, cols_block)
    local_terms = weight_terms(padded_block, cotangent, frames_block, rows_block, cols_block)
    grad_weight = lax.psum_scatter(local_terms, ("tm", "height"), scatter_dimension=0, tiled=True)
    sigmoid = jax.nn.sigmoid(normed_block)
    grad_normed = grad_active * sigmoid * (1.0 + normed_block * (1.0 - sigmoid))
    flat_grad = grad_normed.reshape(-1, channels_block)
    flat_standard = standard.reshape(-1, channels_block)
    grad_shift, grad_gain = lax.psum(
        (jnp.sum(flat_grad, axis=0), jnp.sum(flat_grad * flat_standard, axis=0)), ("tm", "height")
    )
    first_mean = jnp.sum((gain_block * grad_shift).reshape(GROUPS, per_block), axis=1) / count_block
    second_mean = jnp.sum((gain_block * grad_gain).reshape(GROUPS, per_block), axis=1) / count_block
    grouped_grad = (grad_normed * gain_block).reshape(-1, GROUPS, per_block)
    grouped_standard = standard.reshape(-1, GROUPS, per_block)
    corrected = (
        grouped_grad - first_mean[:, None] - grouped_standard * second_mean[:, None]
    ) * inverse_block[:, None]
    grad_upsampled = (cotangent.astype(jnp.float32) + corrected.reshape(cotangent.shape)).astype(
        jnp.bfloat16
    )
    return (decoded, grad_upsampled, grad_weight, grad_gain, grad_shift)


MESH = pl.DeviceIdType.MESH
F32 = jnp.float32
BF16 = jnp.bfloat16


def group_matrix(channels, per):
    row = lax.broadcasted_iota(jnp.int32, (channels, channels), 0) // per
    col = lax.broadcasted_iota(jnp.int32, (channels, channels), 1) // per
    return (row == col).astype(F32)


def over_groups(rows, per):
    return jnp.dot(
        rows,
        group_matrix(rows.shape[-1], per),
        precision=lax.Precision.HIGHEST,
        preferred_element_type=F32,
    )


def column_shift(cells, cols, step):
    count = cells.shape[0]
    column = lax.broadcasted_iota(jnp.int32, cells.shape, 0) % cols
    edge = 0 if step == 1 else cols - 1
    return jnp.where(column == edge, 0.0, pltpu.roll(cells, step % count, 0))


def two_rows(first, second):
    width = first.shape[-1]
    row = lax.broadcasted_iota(jnp.int32, (8, width), 0)
    return jnp.where(row == 0, first, jnp.where(row == 1, second, 0.0))


def block_kernel(sizes, n_send, *refs):
    (T, H, Fl, Rl, Cl, CH, C2, F, R, C) = sizes
    (
        latent, gain_l, shift_l, w_l, up_w, gain_b, shift_b, w_b, cot,
        decoded, grad_up, grad_w, grad_gs,
        act, abuf, acc_l, part, parts_in, stat1, stat2, stat3, upw, wb,
        upf, std, ab, cb, cot3, gw, gy, gs, gz, acc, lace, send_sem, recv_sem, local_sem,
    ) = refs
    d, t, h = lax.axis_index("dp"), lax.axis_index("tm"), lax.axis_index("height")
    N = T * H
    FL = T * Fl
    U = H * CH // T
    band = Rl // H
    pair = d + 1 - 2 * (d % 2)
    half = d % 2
    used = [0]
    sent = []

    def at(kt, kh):
        return (d, lax.rem(t + kt, T), lax.rem(h + kh, H))

    def copy(src, dst, device):
        k = used[0]
        used[0] += 1
        return pltpu.make_async_remote_copy(
            src_ref=src, dst_ref=dst, send_sem=send_sem.at[k], recv_sem=recv_sem.at[k],
            device_id=device, device_id_type=MESH,
        )

    def go(src, dst, device):
        made = copy(src, dst, device)
        made.start()
        sent.append(made)
        return made

    peers = [(kt, kh) for kt in range(T) for kh in range(H) if kt or kh]

    abuf[...] = jnp.zeros(abuf.shape, BF16)
    ab[...] = jnp.zeros(ab.shape, BF16)
    cb[...] = jnp.zeros(cb.shape, BF16)

    barrier = pltpu.get_barrier_semaphore()
    for kt, kh in peers:
        pl.semaphore_signal(barrier, inc=1, device_id=at(kt, kh), device_id_type=MESH)
    pl.semaphore_signal(barrier, inc=1, device_id=(pair, t, h), device_id_type=MESH)
    pl.semaphore_wait(barrier, N)

    x = latent[...].astype(F32).reshape(Fl * Rl * Cl, CH)
    stat1[t] = two_rows(jnp.sum(x, 0, keepdims=True), jnp.sum(x * x, 0, keepdims=True))
    s1 = [go(stat1.at[t], stat1.at[t], at(kt, 0)) for kt in range(1, T)]
    cb[0:F, 1 : 1 + R] = cot[...]
    wide = cot[...].astype(F32).reshape(F * R * C, C2)
    cot3[:, 0:C2] = column_shift(wide, C, -1).astype(BF16)
    cot3[:, C2 : 2 * C2] = cot[...].reshape(F * R * C, C2)
    cot3[:, 2 * C2 :] = column_shift(wide, C, 1).astype(BF16)
    for made in s1:
        made.wait_recv()
    per_l = H * CH // GROUPS
    count_l = FL * Rl * Cl * per_l
    total = stat1[0]
    for k in range(1, T):
        total = total + stat1[k]
    total = over_groups(total, per_l) / count_l
    mean_l = total[0:1]
    inv_l = lax.rsqrt(total[1:2] - mean_l * mean_l + epsilon)
    v = (x - mean_l) * inv_l * gain_l[...] + shift_l[...]
    act[...] = (v * jax.nn.sigmoid(v)).astype(BF16).reshape(Fl, Rl, Cl, CH)
    lane = pl.multiple_of(lax.rem(h * CH, U), CH)
    mine = abuf.at[(h * CH) // U, pl.ds(2 + t * Fl, Fl), pl.ds(1, Rl), :, pl.ds(lane, CH)]
    a_in = [go(act, mine, at(kt, kh)) for kt, kh in peers]
    own_a = pltpu.make_async_copy(act, mine, local_sem.at[0])
    own_a.start()

    up_rows = CH // T
    up_cols = pl.ds(pl.multiple_of(half * (4 * C2), C2), 4 * C2)

    def up_piece(gt, gh):
        return upw.at[pl.ds(pl.multiple_of(gh * CH + gt * up_rows, up_rows), up_rows), up_cols]

    own_rows = up_w.at[pl.ds(pl.multiple_of(t * up_rows, up_rows), up_rows), up_cols]
    up_z = [go(own_rows, up_piece(t, h), at(0, kh)) for kh in range(1, H)]
    own_up = pltpu.make_async_copy(up_w, upw.at[pl.ds(pl.multiple_of(h * CH, CH), CH)], local_sem.at[1])
    own_up.start()

    def halo(buffer, frames_at, step, edge_src):
        made = []
        f_all, f_two, two_at, all_at = frames_at
        ok_t_send = (t < T - 1) if step == 1 else (t > 0)
        ok_t_recv = (t > 0) if step == 1 else (t < T - 1)
        kt = step % T
        for kt_, kh_, ok_s, ok_r, src, dst in (
            (kt, 0, ok_t_send, ok_t_recv, edge_src(f_two, 0, R), buffer.at[pl.ds(two_at, 2), pl.ds(1, R)]),
            (0, 1, h < H - 1, h > 0, edge_src(f_all, R - 1, 1), buffer.at[pl.ds(all_at, F), pl.ds(0, 1)]),
            (0, H - 1, h > 0, h < H - 1, edge_src(f_all, 0, 1), buffer.at[pl.ds(all_at, F), pl.ds(R + 1, 1)]),
            (kt, 1, ok_t_send & (h < H - 1), ok_t_recv & (h > 0),
             edge_src(f_two, R - 1, 1), buffer.at[pl.ds(two_at, 2), pl.ds(0, 1)]),
            (kt, H - 1, ok_t_send & (h > 0), ok_t_recv & (h < H - 1),
             edge_src(f_two, 0, 1), buffer.at[pl.ds(two_at, 2), pl.ds(R + 1, 1)]),
        ):
            c = copy(src, dst, at(kt_, kh_))
            pl.when(ok_s)(c.start)
            made.append((c, ok_s, ok_r))
        return made

    cot_halo = halo(
        cb, ((0, F), (0, 2), F, 0), -1,
        lambda fs, r0, n: cot.at[pl.ds(fs[0], fs[1]), pl.ds(r0, n)],
    )

    acc_l[...] = jnp.zeros(acc_l.shape, F32)
    own_a.wait()
    for made in a_in:
        made.wait_recv()
    cells_l = FL * Rl * Cl

    def latent_tap(j, _):
        unit = t * 27 + j
        tap, chunk = unit // T, unit % T
        lag, dr, dc = tap // 9, (tap // 3) % 3, tap % 3
        win = abuf[chunk, pl.ds(lag, FL), pl.ds(dr, Rl)].reshape(cells_l, U)
        rows = w_l[pl.ds(pl.multiple_of(j * U, U), U), :]
        acc_l[dc] += jnp.dot(win, rows, preferred_element_type=F32)
        return 0

    lax.fori_loop(0, 27, latent_tap, 0)
    mixed = column_shift(acc_l[0], Cl, 1) + acc_l[1] + column_shift(acc_l[2], Cl, -1)
    part[...] = mixed.reshape(FL, Rl, Cl, CH)
    part[pl.ds(t * Fl, Fl)] += latent[...].astype(F32)
    p_in = []
    for kt, kh in peers:
        dev = at(kt, kh)
        p_in.append(
            go(part.at[pl.ds(dev[1] * Fl, Fl), pl.ds(dev[2] * band, band)],
               parts_in.at[kt * H + kh], dev)
        )

    up_pair, up_y = [], []
    for kh in range(1, H):
        up_z[kh - 1].wait_recv()
        got = up_piece(t, lax.rem(h + H - kh, H))
        up_pair.append(go(got, got, (pair, t, h)))
        for kt in range(1, T):
            up_y.append((kt, kh, go(got, got, at(kt, 0))))

    shard = w_b.shape[0]
    w_cols = pl.ds(pl.multiple_of(half * (C2 // 2), C2 // 2), C2 // 2)

    def w_piece(gt, gh):
        return wb.at[pl.ds(pl.multiple_of((gt * H + gh) * shard, shard), shard), w_cols]

    w_z = [go(w_b.at[:, w_cols], w_piece(t, h), at(0, kh)) for kh in range(1, H)]
    w_y = [(kt, 0, go(w_b.at[:, w_cols], w_piece(t, h), at(kt, 0))) for kt in range(1, T)]
    own_w = pltpu.make_async_copy(
        w_b, wb.at[pl.ds(pl.multiple_of((t * H + h) * shard, shard), shard)], local_sem.at[2]
    )
    own_w.start()

    for kt, kh, made in up_y:
        made.wait_recv()
        got = up_piece(lax.rem(t + T - kt, T), lax.rem(h + H - kh, H))
        up_pair.append(go(got, got, (pair, t, h)))
    for made in p_in:
        made.wait_recv()
    own_up.wait()
    for made in up_pair:
        made.wait_recv()

    cells_b = Fl * band * Cl
    parts_own = part[pl.ds(t * Fl, Fl), pl.ds(h * band, band)]
    expanded = jnp.zeros((cells_b, 8 * C2), F32)
    for kh in range(H):
        value = parts_own if kh == 0 else parts_in[kh]
        for kt in range(1, T):
            value = value + parts_in[kt * H + kh]
        refined = value.reshape(cells_b, CH).astype(BF16)
        source = lax.rem(h + H - kh, H)
        expanded = expanded + jnp.dot(
            refined, upw[pl.ds(pl.multiple_of(source * CH, CH), CH), :],
            preferred_element_type=F32,
        )
    expanded = expanded.astype(BF16).astype(F32)
    for f in range(Fl):
        for r in range(band):
            for p in range(2):
                for q in range(2):
                    for s in range(2):
                        first = (f * band + r) * Cl
                        col = ((p * 2 + q) * 2 + s) * C2
                        for n in range(C2 // 128):
                            lace[
                                n, pl.ds(((2 * f + p) * R + 2 * r + q) * C + s, Cl, stride=2), :
                            ] = expanded[first : first + Cl, col + n * 128 : col + (n + 1) * 128]

    cells = F * R * C
    me = t * H + h
    up = jnp.concatenate([lace[n] for n in range(C2 // 128)], axis=1)
    upf[...] = up
    stat2[me] = two_rows(jnp.sum(up, 0, keepdims=True), jnp.sum(up * up, 0, keepdims=True))
    s2 = [go(stat2.at[me], stat2.at[me], at(kt, kh)) for kt, kh in peers]
    for made in s2:
        made.wait_recv()
    per_b = C2 // GROUPS
    count_b = cells * per_b * N
    total = stat2[0]
    for k in range(1, N):
        total = total + stat2[k]
    total = over_groups(total, per_b) / count_b
    mean_b = total[0:1]
    inv_b = lax.rsqrt(total[1:2] - mean_b * mean_b + epsilon)
    standard = (up - mean_b) * inv_b
    std[...] = standard
    normed = standard * gain_b[...] + shift_b[...]
    ab[2 : 2 + F, 1 : 1 + R] = (
        (normed * jax.nn.sigmoid(normed)).astype(BF16).reshape(F, R, C, C2)
    )
    ab_halo = halo(
        ab, ((2, F), (F, 2), 0, 2), 1,
        lambda fs, r0, n: ab.at[pl.ds(fs[0], fs[1]), pl.ds(1 + r0, n)],
    )

    w_pair = []
    for kh in range(1, H):
        w_z[kh - 1].wait_recv()
        got = w_piece(t, lax.rem(h + H - kh, H))
        w_pair.append(go(got, got, (pair, t, h)))
        for kt in range(1, T):
            w_y.append((kt, kh, go(got, got, at(kt, 0))))

    for made, _, ok in ab_halo:
        pl.when(ok)(made.wait_recv)

    for dr in range(3):
        win = ab[2 : 2 + F, dr : dr + R].reshape(cells, C2)
        for dc in range(3):
            term = lax.dot_general(
                win, cot3[:, dc * C2 : (dc + 1) * C2],
                (((0,), (0,)), ((), ())), preferred_element_type=F32,
            )
            gw[(dr * 3 + dc) * C2 : (dr * 3 + dc + 1) * C2, :] = term.astype(BF16)
    out_rows = 9 * C2 // N
    y_rows = out_rows * H
    g_y = []
    for kt in range(1, T):
        dev = at(kt, 0)
        g_y.append(go(gw.at[pl.ds(pl.multiple_of(dev[1] * y_rows, y_rows), y_rows)], gy.at[kt], dev))

    for kt, kh, made in w_y:
        made.wait_recv()
        got = w_piece(lax.rem(t + T - kt, T), lax.rem(h + H - kh, H))
        w_pair.append(go(got, got, (pair, t, h)))
    for made, _, ok in cot_halo:
        pl.when(ok)(made.wait_recv)
    own_w.wait()
    for made in w_pair:
        made.wait_recv()
    for made in g_y:
        made.wait_recv()
    summed = gw[pl.ds(pl.multiple_of(t * y_rows, y_rows), y_rows), :].astype(F32)
    for kt in range(1, T):
        summed = summed + gy[kt].astype(F32)
    gs[...] = summed.astype(BF16)
    g_z = []
    for kh in range(1, H):
        dev = at(0, kh)
        g_z.append(go(gs.at[pl.ds(pl.multiple_of(dev[2] * out_rows, out_rows), out_rows)], gz.at[kh], dev))

    acc[...] = jnp.zeros(acc.shape, F32)

    def grad_tap(j, _):
        lag, dr = j // 3, j % 3
        win = cb[pl.ds(2 - lag, F), pl.ds(2 - dr, R)].reshape(cells, C2)
        for dc in range(3):
            rows = wb[pl.ds(pl.multiple_of((j * 3 + dc) * C2, C2), C2), :]
            acc[dc] += lax.dot_general(
                win, rows, (((1,), (1,)), ((), ())), preferred_element_type=F32
            )
        return 0

    lax.fori_loop(0, 9, grad_tap, 0)
    grad_active = column_shift(acc[0], C, -1) + acc[1] + column_shift(acc[2], C, 1)
    standard = std[...]
    normed = standard * gain_b[...] + shift_b[...]
    sigmoid = jax.nn.sigmoid(normed)
    grad_normed = grad_active * sigmoid * (1.0 + normed * (1.0 - sigmoid))
    stat3[me] = two_rows(
        jnp.sum(grad_normed * standard, 0, keepdims=True), jnp.sum(grad_normed, 0, keepdims=True)
    )
    s3 = [go(stat3.at[me], stat3.at[me], at(kt, kh)) for kt, kh in peers]
    upf_keep = upf[...]
    upf[...] = grad_normed * gain_b[...]

    acc[...] = jnp.zeros(acc.shape, F32)

    def tap(j, _):
        lag, dr = j // 3, j % 3
        win = ab[pl.ds(lag, F), pl.ds(dr, R)].reshape(cells, C2)
        for dc in range(3):
            rows = wb[pl.ds(pl.multiple_of((j * 3 + dc) * C2, C2), C2), :]
            acc[dc] += jnp.dot(win, rows, preferred_element_type=F32)
        return 0

    acc[1] = upf_keep
    lax.fori_loop(0, 9, tap, 0)
    decoded[...] = (
        (column_shift(acc[0], C, 1) + acc[1] + column_shift(acc[2], C, -1))
        .astype(BF16).reshape(F, R, C, C2)
    )

    for made in s3:
        made.wait_recv()
    total = stat3[0]
    for k in range(1, N):
        total = total + stat3[k]
    grad_gs[...] = total
    means = over_groups(total * gain_b[...], per_b) / count_b
    corrected = (upf[...] - means[1:2] - std[...] * means[0:1]) * inv_b
    grad_up[...] = (
        cot[...].astype(F32).reshape(cells, C2) + corrected
    ).astype(BF16).reshape(F, R, C, C2)

    for made in g_z:
        made.wait_recv()
    result = gs[pl.ds(pl.multiple_of(h * out_rows, out_rows), out_rows), :].astype(F32)
    for kh in range(1, H):
        result = result + gz[kh].astype(F32)
    grad_w[...] = result

    for made in sent:
        made.wait_send()
    for made, ok, _ in cot_halo + ab_halo:
        pl.when(ok)(made.wait_send)
    assert used[0] <= n_send


def local_block(shape, *args):
    (latent, gain_l, shift_l, w_l, up_w, gain_b, shift_b, w_b, cot) = args
    T, H = shape["tm"], shape["height"]
    Fl, Rl, Cl, CH = latent.shape
    F, R, C, C2 = cot.shape
    N = T * H
    U = H * CH // T
    fits = (
        shape["dp"] % 2 == 0
        and CH % 128 == 0 and U % CH == 0
        and w_b.shape[0] % 16 == 0 and (CH // T) % 16 == 0
        and (9 * C2) % (16 * N) == 0 and C2 % 256 == 0
        and Cl % 16 == 0 and w_l.shape[0] == 27 * U and F >= 2
    )
    if not fits:
        return local(*args)
    sizes = (T, H, Fl, Rl, Cl, CH, C2, F, R, C)
    n_send = 16 + 4 * T + 4 * N + 6 * N + 3 * N
    FL = T * Fl
    band = Rl // H
    cells = F * R * C
    out_rows = 9 * C2 // N
    vmem = pl.BlockSpec(memory_space=pltpu.VMEM)
    flops = 2 * (FL * Rl * Cl * w_l.size + 2 * cells * 27 * C2 * C2 + cells * 9 * C2 * C2)
    outs = pl.pallas_call(
        functools.partial(block_kernel, sizes, n_send),
        out_shape=(
            jax.ShapeDtypeStruct(cot.shape, BF16),
            jax.ShapeDtypeStruct(cot.shape, BF16),
            jax.ShapeDtypeStruct((out_rows, C2), F32),
            jax.ShapeDtypeStruct((8, C2), F32),
        ),
        in_specs=[vmem] * 9,
        out_specs=(vmem,) * 4,
        scratch_shapes=[
            pltpu.VMEM((Fl, Rl, Cl, CH), BF16),
            pltpu.VMEM((T, FL + 2, Rl + 2, Cl, U), BF16),
            pltpu.VMEM((3, FL * Rl * Cl, CH), F32),
            pltpu.VMEM((FL, Rl, Cl, CH), F32),
            pltpu.VMEM((N, Fl, band, Cl, CH), F32),
            pltpu.VMEM((T, 8, CH), F32),
            pltpu.VMEM((N, 8, C2), F32),
            pltpu.VMEM((N, 8, C2), F32),
            pltpu.VMEM((H * CH, 8 * C2), BF16),
            pltpu.VMEM((27 * C2, C2), BF16),
            pltpu.VMEM((cells, C2), F32),
            pltpu.VMEM((cells, C2), F32),
            pltpu.VMEM((F + 2, R + 2, C, C2), BF16),
            pltpu.VMEM((F + 2, R + 2, C, C2), BF16),
            pltpu.VMEM((cells, 3 * C2), BF16),
            pltpu.VMEM((9 * C2, C2), BF16),
            pltpu.VMEM((T, out_rows * H, C2), BF16),
            pltpu.VMEM((out_rows * H, C2), BF16),
            pltpu.VMEM((H, out_rows, C2), BF16),
            pltpu.VMEM((3, cells, C2), F32),
            pltpu.VMEM((C2 // 128, cells, 128), F32),
            pltpu.SemaphoreType.DMA((n_send,)),
            pltpu.SemaphoreType.DMA((n_send,)),
            pltpu.SemaphoreType.DMA((3,)),
        ],
        compiler_params=pltpu.CompilerParams(
            collective_id=0, has_side_effects=True, vmem_limit_bytes=60 * 1024 * 1024
        ),
        cost_estimate=pl.CostEstimate(flops=flops, bytes_accessed=1 << 23, transcendentals=0),
    )(
        latent, gain_l.reshape(1, -1), shift_l.reshape(1, -1), w_l, up_w,
        gain_b.reshape(1, -1), shift_b.reshape(1, -1), w_b, cot,
    )
    decoded, grad_up, grad_w, grad_gs = outs
    return decoded, grad_up, grad_w, grad_gs[0], grad_gs[1]


def solution(mesh):
    return jax.shard_map(
        functools.partial(local_block, dict(mesh.shape)),
        mesh=mesh,
        in_specs=(
            P(("dp", "tm"), None, None, "height"),
            P("height"),
            P("height"),
            P("tm", "height"),
            P("height", None),
            P(),
            P(),
            P(("tm", "height"), None),
            P(("dp", "tm"), "height", None, None),
        ),
        out_specs=(
            P(("dp", "tm"), "height", None, None),
            P(("dp", "tm"), "height", None, None),
            P(("dp", "tm", "height"), None),
            P("dp"),
            P("dp"),
        ),
        check_vma=False,
    )
```

```python
import functools

import jax
import jax.numpy as jnp
from jax import lax
from jax.experimental import pallas as pl
from jax.experimental.pallas import tpu as pltpu
from jax.sharding import PartitionSpec as P

C1 = 512
GROUPS = 32


epsilon = 1e-06


def shifted(block, axis, distance):
    devices = range(lax.axis_size(axis))
    route = [(i - distance, i) for i in devices if i - distance in devices]
    return lax.ppermute(block, axis, route)


def extended_2(cells, sides, width):
    for axis, dim in sides:
        count = lax.axis_size(axis)
        ends = count - 1
        head = lax.slice_in_dim(cells, 0, width, axis=dim)
        tail = lax.slice_in_dim(cells, cells.shape[dim] - width, cells.shape[dim], axis=dim)
        cells = jnp.concatenate(
            [
                lax.ppermute(tail, axis, [(i, (i + 1) % count) for i in range(ends)]),
                cells,
                lax.ppermute(head, axis, [((i + 1) % count, i) for i in range(ends)]),
            ],
            axis=dim,
        )
    return cells


def standardize(values, mean_value, inverse, groups):
    shape_full = values.shape
    grouped = values.reshape(shape_full[:-1] + (groups, shape_full[-1] // groups))
    return ((grouped - mean_value[:, None]) * inverse[:, None]).reshape(shape_full)


def causal_taps(padded, weight, frames, rows, cols):
    channels_in = padded.shape[-1]
    summed = jnp.zeros((frames * rows * cols, weight.shape[1]), jnp.float32)
    for lag_step in range(3):
        for row_step in range(3):
            for col_step in range(3):
                tap_index = (lag_step * 3 + row_step) * 3 + col_step
                window = padded[
                    lag_step : lag_step + frames,
                    row_step : row_step + rows,
                    col_step : col_step + cols,
                ]
                kernel = weight[tap_index * channels_in : (tap_index + 1) * channels_in]
                summed = summed + jnp.dot(
                    window.reshape(-1, channels_in), kernel, preferred_element_type=jnp.float32
                )
    return summed.reshape(frames, rows, cols, weight.shape[1])


def transposed_taps(padded, weight, frames, rows, cols):
    channels_out = padded.shape[-1]
    channels_in = weight.shape[0] // 27
    summed = jnp.zeros((frames * rows * cols, channels_in), jnp.float32)
    for lag_step in range(3):
        for row_step in range(3):
            for col_step in range(3):
                tap_index = (lag_step * 3 + row_step) * 3 + col_step
                window = padded[
                    2 - lag_step : 2 - lag_step + frames,
                    2 - row_step : 2 - row_step + rows,
                    2 - col_step : 2 - col_step + cols,
                ]
                kernel = weight[tap_index * channels_in : (tap_index + 1) * channels_in]
                summed = summed + lax.dot_general(
                    window.reshape(-1, channels_out),
                    kernel,
                    (((1,), (1,)), ((), ())),
                    preferred_element_type=jnp.float32,
                )
    return summed.reshape(frames, rows, cols, channels_in)


def weight_terms(padded, grads, frames, rows, cols):
    channels_in = padded.shape[-1]
    flat_grads = grads.reshape(-1, grads.shape[-1])
    blocks = []
    for row_step in range(3):
        for col_step in range(3):
            window = padded[2 : 2 + frames, row_step : row_step + rows, col_step : col_step + cols]
            blocks.append(
                lax.dot_general(
                    window.reshape(-1, channels_in),
                    flat_grads,
                    (((0,), (0,)), ((), ())),
                    preferred_element_type=jnp.float32,
                )
            )
    return jnp.concatenate(blocks, 0)


def local(
    latent,
    gain_latent,
    shift_latent,
    conv_latent,
    up_weight,
    gain_block,
    shift_block,
    conv_block,
    cotangent,
):
    per_group = C1 // GROUPS
    groups_here = latent.shape[-1] // per_group
    latent_f32 = latent.astype(jnp.float32)
    grouped = latent_f32.reshape(-1, groups_here, per_group)
    first_sums = jnp.sum(grouped, axis=(0, 2))
    second_sums = jnp.sum(grouped * grouped, axis=(0, 2))
    first_totals, second_totals = lax.psum((first_sums, second_sums), "tm")
    count_latent = grouped.shape[0] * per_group * lax.axis_size("tm")
    mean_latent = first_totals / count_latent
    inverse_latent = lax.rsqrt(second_totals / count_latent - mean_latent * mean_latent + epsilon)
    normed = (
        standardize(latent_f32, mean_latent, inverse_latent, groups_here) * gain_latent
        + shift_latent
    )
    active = jax.nn.silu(normed).astype(jnp.bfloat16)
    earlier = shifted(active, "tm", 1)
    extended = jnp.concatenate([earlier, active], 0)
    all_channels = lax.all_gather(extended, "height", axis=3, tiled=True)
    padded = jnp.pad(all_channels, ((0, 0), (1, 1), (1, 1), (0, 0)))
    latent_weight = lax.all_gather(conv_latent, "tm", axis=0, tiled=True)
    frames_latent, rows_latent, cols_latent = (latent.shape[0], latent.shape[1], latent.shape[2])
    mixed = causal_taps(padded, latent_weight, frames_latent, rows_latent, cols_latent)
    refined = (latent_f32 + mixed).astype(jnp.bfloat16)
    band_rows = rows_latent // lax.axis_size("height")
    own_band = lax.all_to_all(refined, "height", split_axis=1, concat_axis=3, tiled=True)
    flat_band = own_band.reshape(-1, own_band.shape[-1])
    expanded = jnp.dot(
        flat_band,
        lax.all_gather(up_weight, "height", axis=0, tiled=True),
        preferred_element_type=jnp.float32,
    )
    channels_block = up_weight.shape[1] // 8
    spread = expanded.reshape(frames_latent, band_rows, cols_latent, 2, 2, 2, channels_block)
    spread = spread.transpose(0, 3, 1, 4, 2, 5, 6)
    upsampled = spread.reshape(
        2 * frames_latent, 2 * band_rows, 2 * cols_latent, channels_block
    ).astype(jnp.bfloat16)
    frames_block, rows_block, cols_block = (
        upsampled.shape[0],
        upsampled.shape[1],
        upsampled.shape[2],
    )
    up_f32 = upsampled.astype(jnp.float32)
    per_block = channels_block // GROUPS
    grouped_block = up_f32.reshape(-1, GROUPS, per_block)
    block_first = jnp.sum(grouped_block, axis=(0, 2))
    block_second = jnp.sum(grouped_block * grouped_block, axis=(0, 2))
    block_first, block_second = lax.psum((block_first, block_second), ("tm", "height"))
    count_block = grouped_block.shape[0] * per_block * lax.axis_size("tm") * lax.axis_size("height")
    mean_block = block_first / count_block
    inverse_block = lax.rsqrt(block_second / count_block - mean_block * mean_block + epsilon)
    standard = standardize(up_f32, mean_block, inverse_block, GROUPS)
    normed_block = standard * gain_block + shift_block
    active_block = jax.nn.silu(normed_block).astype(jnp.bfloat16)
    before = shifted(active_block[-2:], "tm", 1)
    ext_block = jnp.concatenate([before, active_block], 0)
    beside_all = extended_2(ext_block, (("height", 1),), 1)
    padded_block = jnp.pad(beside_all, ((0, 0), (0, 0), (1, 1), (0, 0)))
    block_weight = lax.all_gather(conv_block, ("tm", "height"), axis=0, tiled=True)
    mixed_block = causal_taps(padded_block, block_weight, frames_block, rows_block, cols_block)
    decoded = (up_f32 + mixed_block).astype(jnp.bfloat16)
    after = shifted(cotangent[:2], "tm", -1)
    grad_ext = jnp.concatenate([cotangent, after], 0)
    grad_around = extended_2(grad_ext, (("height", 1),), 1)
    grad_padded = jnp.pad(grad_around, ((0, 0), (0, 0), (1, 1), (0, 0)))
    grad_active = transposed_taps(grad_padded, block_weight, frames_block, rows_block, cols_block)
    local_terms = weight_terms(padded_block, cotangent, frames_block, rows_block, cols_block)
    grad_weight = lax.psum_scatter(local_terms, ("tm", "height"), scatter_dimension=0, tiled=True)
    sigmoid = jax.nn.sigmoid(normed_block)
    grad_normed = grad_active * sigmoid * (1.0 + normed_block * (1.0 - sigmoid))
    flat_grad = grad_normed.reshape(-1, channels_block)
    flat_standard = standard.reshape(-1, channels_block)
    grad_shift, grad_gain = lax.psum(
        (jnp.sum(flat_grad, axis=0), jnp.sum(flat_grad * flat_standard, axis=0)), ("tm", "height")
    )
    first_mean = jnp.sum((gain_block * grad_shift).reshape(GROUPS, per_block), axis=1) / count_block
    second_mean = jnp.sum((gain_block * grad_gain).reshape(GROUPS, per_block), axis=1) / count_block
    grouped_grad = (grad_normed * gain_block).reshape(-1, GROUPS, per_block)
    grouped_standard = standard.reshape(-1, GROUPS, per_block)
    corrected = (
        grouped_grad - first_mean[:, None] - grouped_standard * second_mean[:, None]
    ) * inverse_block[:, None]
    grad_upsampled = (cotangent.astype(jnp.float32) + corrected.reshape(cotangent.shape)).astype(
        jnp.bfloat16
    )
    return (decoded, grad_upsampled, grad_weight, grad_gain, grad_shift)


MESH = pl.DeviceIdType.MESH
F32 = jnp.float32
BF16 = jnp.bfloat16


def group_matrix(channels, per):
    row = lax.broadcasted_iota(jnp.int32, (channels, channels), 0) // per
    col = lax.broadcasted_iota(jnp.int32, (channels, channels), 1) // per
    return (row == col).astype(F32)


def over_groups(rows, per):
    return jnp.dot(
        rows,
        group_matrix(rows.shape[-1], per),
        precision=lax.Precision.HIGHEST,
        preferred_element_type=F32,
    )


def column_shift(cells, cols, step):
    count = cells.shape[0]
    column = lax.broadcasted_iota(jnp.int32, cells.shape, 0) % cols
    edge = 0 if step == 1 else cols - 1
    return jnp.where(column == edge, 0.0, pltpu.roll(cells, step % count, 0))


def two_rows(first, second):
    width = first.shape[-1]
    row = lax.broadcasted_iota(jnp.int32, (8, width), 0)
    return jnp.where(row == 0, first, jnp.where(row == 1, second, 0.0))


def block_kernel(sizes, n_send, *refs):
    (T, H, Fl, Rl, Cl, CH, C2, F, R, C) = sizes
    (
        latent, gain_l, shift_l, w_l, up_w, gain_b, shift_b, w_b, cot,
        decoded, grad_up, grad_w, grad_gs,
        act, abuf, acc_l, part, parts_in, stat1, stat2, stat3, upw, wb,
        upf, std, ab, cb, cot3, gw, gy, gs, gz, acc, lace, send_sem, recv_sem, local_sem,
    ) = refs
    d, t, h = lax.axis_index("dp"), lax.axis_index("tm"), lax.axis_index("height")
    N = T * H
    FL = T * Fl
    U = H * CH // T
    band = Rl // H
    pair = d + 1 - 2 * (d % 2)
    half = d % 2
    used = [0]
    sent = []

    def at(kt, kh):
        return (d, lax.rem(t + kt, T), lax.rem(h + kh, H))

    def copy(src, dst, device):
        k = used[0]
        used[0] += 1
        return pltpu.make_async_remote_copy(
            src_ref=src, dst_ref=dst, send_sem=send_sem.at[k], recv_sem=recv_sem.at[k],
            device_id=device, device_id_type=MESH,
        )

    def go(src, dst, device):
        made = copy(src, dst, device)
        made.start()
        sent.append(made)
        return made

    peers = [(kt, kh) for kt in range(T) for kh in range(H) if kt or kh]

    abuf[...] = jnp.zeros(abuf.shape, BF16)
    ab[...] = jnp.zeros(ab.shape, BF16)
    cb[...] = jnp.zeros(cb.shape, BF16)

    barrier = pltpu.get_barrier_semaphore()
    for kt, kh in peers:
        pl.semaphore_signal(barrier, inc=1, device_id=at(kt, kh), device_id_type=MESH)
    pl.semaphore_signal(barrier, inc=1, device_id=(pair, t, h), device_id_type=MESH)
    pl.semaphore_wait(barrier, N)

    x = latent[...].astype(F32).reshape(Fl * Rl * Cl, CH)
    stat1[t] = two_rows(jnp.sum(x, 0, keepdims=True), jnp.sum(x * x, 0, keepdims=True))
    s1 = [go(stat1.at[t], stat1.at[t], at(kt, 0)) for kt in range(1, T)]
    cb[0:F, 1 : 1 + R] = cot[...]
    wide = cot[...].astype(F32).reshape(F * R * C, C2)
    cot3[:, 0:C2] = column_shift(wide, C, -1).astype(BF16)
    cot3[:, C2 : 2 * C2] = cot[...].reshape(F * R * C, C2)
    cot3[:, 2 * C2 :] = column_shift(wide, C, 1).astype(BF16)
    for made in s1:
        made.wait_recv()
    per_l = H * CH // GROUPS
    count_l = FL * Rl * Cl * per_l
    total = stat1[0]
    for k in range(1, T):
        total = total + stat1[k]
    total = over_groups(total, per_l) / count_l
    mean_l = total[0:1]
    inv_l = lax.rsqrt(total[1:2] - mean_l * mean_l + epsilon)
    v = (x - mean_l) * inv_l * gain_l[...] + shift_l[...]
    act[...] = (v * jax.nn.sigmoid(v)).astype(BF16).reshape(Fl, Rl, Cl, CH)
    lane = pl.multiple_of(lax.rem(h * CH, U), CH)
    mine = abuf.at[(h * CH) // U, pl.ds(2 + t * Fl, Fl), pl.ds(1, Rl), :, pl.ds(lane, CH)]
    a_in = [go(act, mine, at(kt, kh)) for kt, kh in peers]
    own_a = pltpu.make_async_copy(act, mine, local_sem.at[0])
    own_a.start()

    up_rows = CH // T
    up_cols = pl.ds(pl.multiple_of(half * (4 * C2), C2), 4 * C2)

    def up_piece(gt, gh):
        return upw.at[pl.ds(pl.multiple_of(gh * CH + gt * up_rows, up_rows), up_rows), up_cols]

    own_rows = up_w.at[pl.ds(pl.multiple_of(t * up_rows, up_rows), up_rows), up_cols]
    up_z = [go(own_rows, up_piece(t, h), at(0, kh)) for kh in range(1, H)]
    own_up = pltpu.make_async_copy(up_w, upw.at[pl.ds(pl.multiple_of(h * CH, CH), CH)], local_sem.at[1])
    own_up.start()

    def halo(buffer, frames_at, step, edge_src):
        made = []
        f_all, f_two, two_at, all_at = frames_at
        ok_t_send = (t < T - 1) if step == 1 else (t > 0)
        ok_t_recv = (t > 0) if step == 1 else (t < T - 1)
        kt = step % T
        for kt_, kh_, ok_s, ok_r, src, dst in (
            (kt, 0, ok_t_send, ok_t_recv, edge_src(f_two, 0, R), buffer.at[pl.ds(two_at, 2), pl.ds(1, R)]),
            (0, 1, h < H - 1, h > 0, edge_src(f_all, R - 1, 1), buffer.at[pl.ds(all_at, F), pl.ds(0, 1)]),
            (0, H - 1, h > 0, h < H - 1, edge_src(f_all, 0, 1), buffer.at[pl.ds(all_at, F), pl.ds(R + 1, 1)]),
            (kt, 1, ok_t_send & (h < H - 1), ok_t_recv & (h > 0),
             edge_src(f_two, R - 1, 1), buffer.at[pl.ds(two_at, 2), pl.ds(0, 1)]),
            (kt, H - 1, ok_t_send & (h > 0), ok_t_recv & (h < H - 1),
             edge_src(f_two, 0, 1), buffer.at[pl.ds(two_at, 2), pl.ds(R + 1, 1)]),
        ):
            c = copy(src, dst, at(kt_, kh_))
            pl.when(ok_s)(c.start)
            made.append((c, ok_s, ok_r))
        return made

    cot_halo = halo(
        cb, ((0, F), (0, 2), F, 0), -1,
        lambda fs, r0, n: cot.at[pl.ds(fs[0], fs[1]), pl.ds(r0, n)],
    )

    shard = w_b.shape[0]
    w_cols = pl.ds(pl.multiple_of(half * (C2 // 2), C2 // 2), C2 // 2)

    def w_piece(gt, gh):
        return wb.at[pl.ds(pl.multiple_of((gt * H + gh) * shard, shard), shard), w_cols]

    w_z = [go(w_b.at[:, w_cols], w_piece(t, h), at(0, 1))]
    w_y = [(kt, 0, go(w_b.at[:, w_cols], w_piece(t, h), at(kt, 0))) for kt in range(1, T)]
    own_w = pltpu.make_async_copy(
        w_b, wb.at[pl.ds(pl.multiple_of((t * H + h) * shard, shard), shard)], local_sem.at[2]
    )
    own_w.start()

    acc_l[...] = jnp.zeros(acc_l.shape, F32)
    own_a.wait()
    for made in a_in:
        made.wait_recv()
    cells_l = FL * Rl * Cl

    def latent_tap(j, _):
        unit = t * 27 + j
        tap, chunk = unit // T, unit % T
        lag, dr, dc = tap // 9, (tap // 3) % 3, tap % 3
        win = abuf[chunk, pl.ds(lag, FL), pl.ds(dr, Rl)].reshape(cells_l, U)
        rows = w_l[pl.ds(pl.multiple_of(j * U, U), U), :]
        acc_l[dc] += jnp.dot(win, rows, preferred_element_type=F32)
        return 0

    lax.fori_loop(0, 27, latent_tap, 0)
    mixed = column_shift(acc_l[0], Cl, 1) + acc_l[1] + column_shift(acc_l[2], Cl, -1)
    part[...] = mixed.reshape(FL, Rl, Cl, CH)
    part[pl.ds(t * Fl, Fl)] += latent[...].astype(F32)
    p_in = []
    for kt, kh in peers:
        dev = at(kt, kh)
        p_in.append(
            go(part.at[pl.ds(dev[1] * Fl, Fl), pl.ds(dev[2] * band, band)],
               parts_in.at[kt * H + kh], dev)
        )

    up_pair, up_y = [], []
    for kh in range(1, H):
        up_z[kh - 1].wait_recv()
        got = up_piece(t, lax.rem(h + H - kh, H))
        up_pair.append(go(got, got, (pair, t, h)))
        for kt in range(1, T):
            up_y.append((kt, kh, go(got, got, at(kt, 0))))

    w_z += [go(w_b.at[:, w_cols], w_piece(t, h), at(0, kh)) for kh in range(2, H)]

    for kt, kh, made in up_y:
        made.wait_recv()
        got = up_piece(lax.rem(t + T - kt, T), lax.rem(h + H - kh, H))
        up_pair.append(go(got, got, (pair, t, h)))
    for made in p_in:
        made.wait_recv()
    w_pair = []

    def w_onward(kh):
        w_z[kh - 1].wait_recv()
        got = w_piece(t, lax.rem(h + H - kh, H))
        w_pair.append(go(got, got, (pair, t, h)))
        for kt in range(1, T):
            w_y.append((kt, kh, go(got, got, at(kt, 0))))

    w_onward(1)
    own_up.wait()
    for made in up_pair:
        made.wait_recv()

    cells_b = Fl * band * Cl
    parts_own = part[pl.ds(t * Fl, Fl), pl.ds(h * band, band)]
    expanded = jnp.zeros((cells_b, 8 * C2), F32)
    for kh in range(H):
        value = parts_own if kh == 0 else parts_in[kh]
        for kt in range(1, T):
            value = value + parts_in[kt * H + kh]
        refined = value.reshape(cells_b, CH).astype(BF16)
        source = lax.rem(h + H - kh, H)
        expanded = expanded + jnp.dot(
            refined, upw[pl.ds(pl.multiple_of(source * CH, CH), CH), :],
            preferred_element_type=F32,
        )
    expanded = expanded.astype(BF16).astype(F32)
    for f in range(Fl):
        for r in range(band):
            for p in range(2):
                for q in range(2):
                    for s in range(2):
                        first = (f * band + r) * Cl
                        col = ((p * 2 + q) * 2 + s) * C2
                        for n in range(C2 // 128):
                            lace[
                                n, pl.ds(((2 * f + p) * R + 2 * r + q) * C + s, Cl, stride=2), :
                            ] = expanded[first : first + Cl, col + n * 128 : col + (n + 1) * 128]

    cells = F * R * C
    me = t * H + h
    up = jnp.concatenate([lace[n] for n in range(C2 // 128)], axis=1)
    upf[...] = up
    stat2[me] = two_rows(jnp.sum(up, 0, keepdims=True), jnp.sum(up * up, 0, keepdims=True))
    s2 = [go(stat2.at[me], stat2.at[me], at(kt, kh)) for kt, kh in peers]
    for made in s2:
        made.wait_recv()
    per_b = C2 // GROUPS
    count_b = cells * per_b * N
    total = stat2[0]
    for k in range(1, N):
        total = total + stat2[k]
    total = over_groups(total, per_b) / count_b
    mean_b = total[0:1]
    inv_b = lax.rsqrt(total[1:2] - mean_b * mean_b + epsilon)
    standard = (up - mean_b) * inv_b
    std[...] = standard
    normed = standard * gain_b[...] + shift_b[...]
    ab[2 : 2 + F, 1 : 1 + R] = (
        (normed * jax.nn.sigmoid(normed)).astype(BF16).reshape(F, R, C, C2)
    )
    ab_halo = halo(
        ab, ((2, F), (F, 2), 0, 2), 1,
        lambda fs, r0, n: ab.at[pl.ds(fs[0], fs[1]), pl.ds(1 + r0, n)],
    )

    for kh in range(2, H):
        w_onward(kh)

    for made, _, ok in ab_halo:
        pl.when(ok)(made.wait_recv)

    for dr in range(3):
        win = ab[2 : 2 + F, dr : dr + R].reshape(cells, C2)
        for dc in range(3):
            term = lax.dot_general(
                win, cot3[:, dc * C2 : (dc + 1) * C2],
                (((0,), (0,)), ((), ())), preferred_element_type=F32,
            )
            gw[(dr * 3 + dc) * C2 : (dr * 3 + dc + 1) * C2, :] = term.astype(BF16)
    out_rows = 9 * C2 // N
    y_rows = out_rows * H
    g_y = []
    for kt in range(1, T):
        dev = at(kt, 0)
        g_y.append(go(gw.at[pl.ds(pl.multiple_of(dev[1] * y_rows, y_rows), y_rows)], gy.at[kt], dev))

    for kt, kh, made in w_y:
        made.wait_recv()
        got = w_piece(lax.rem(t + T - kt, T), lax.rem(h + H - kh, H))
        w_pair.append(go(got, got, (pair, t, h)))
    for made, _, ok in cot_halo:
        pl.when(ok)(made.wait_recv)
    own_w.wait()
    for made in w_pair:
        made.wait_recv()

    acc[...] = jnp.zeros(acc.shape, F32)

    def grad_tap(j, _):
        lag, dr = j // 3, j % 3
        win = cb[pl.ds(2 - lag, F), pl.ds(2 - dr, R)].reshape(cells, C2)
        for dc in range(3):
            rows = wb[pl.ds(pl.multiple_of((j * 3 + dc) * C2, C2), C2), :]
            acc[dc] += lax.dot_general(
                win, rows, (((1,), (1,)), ((), ())), preferred_element_type=F32
            )
        return 0

    lax.fori_loop(0, 9, grad_tap, 0)
    grad_active = column_shift(acc[0], C, -1) + acc[1] + column_shift(acc[2], C, 1)
    standard = std[...]
    normed = standard * gain_b[...] + shift_b[...]
    sigmoid = jax.nn.sigmoid(normed)
    grad_normed = grad_active * sigmoid * (1.0 + normed * (1.0 - sigmoid))
    stat3[me] = two_rows(
        jnp.sum(grad_normed * standard, 0, keepdims=True), jnp.sum(grad_normed, 0, keepdims=True)
    )
    s3 = [go(stat3.at[me], stat3.at[me], at(kt, kh)) for kt, kh in peers]
    for made in g_y:
        made.wait_recv()
    summed = gw[pl.ds(pl.multiple_of(t * y_rows, y_rows), y_rows), :].astype(F32)
    for kt in range(1, T):
        summed = summed + gy[kt].astype(F32)
    gs[...] = summed.astype(BF16)
    g_z = []
    for kh in range(1, H):
        dev = at(0, kh)
        g_z.append(go(gs.at[pl.ds(pl.multiple_of(dev[2] * out_rows, out_rows), out_rows)], gz.at[kh], dev))

    upf_keep = upf[...]
    upf[...] = grad_normed * gain_b[...]

    acc[...] = jnp.zeros(acc.shape, F32)

    def tap(j, _):
        lag, dr = j // 3, j % 3
        win = ab[pl.ds(lag, F), pl.ds(dr, R)].reshape(cells, C2)
        for dc in range(3):
            rows = wb[pl.ds(pl.multiple_of((j * 3 + dc) * C2, C2), C2), :]
            acc[dc] += jnp.dot(win, rows, preferred_element_type=F32)
        return 0

    acc[1] = upf_keep
    lax.fori_loop(0, 9, tap, 0)
    decoded[...] = (
        (column_shift(acc[0], C, 1) + acc[1] + column_shift(acc[2], C, -1))
        .astype(BF16).reshape(F, R, C, C2)
    )

    for made in s3:
        made.wait_recv()
    total = stat3[0]
    for k in range(1, N):
        total = total + stat3[k]
    grad_gs[...] = total
    means = over_groups(total * gain_b[...], per_b) / count_b
    corrected = (upf[...] - means[1:2] - std[...] * means[0:1]) * inv_b
    grad_up[...] = (
        cot[...].astype(F32).reshape(cells, C2) + corrected
    ).astype(BF16).reshape(F, R, C, C2)

    for made in g_z:
        made.wait_recv()
    result = gs[pl.ds(pl.multiple_of(h * out_rows, out_rows), out_rows), :].astype(F32)
    for kh in range(1, H):
        result = result + gz[kh].astype(F32)
    grad_w[...] = result

    for made in sent:
        made.wait_send()
    for made, ok, _ in cot_halo + ab_halo:
        pl.when(ok)(made.wait_send)
    assert used[0] <= n_send


def local_block(shape, *args):
    (latent, gain_l, shift_l, w_l, up_w, gain_b, shift_b, w_b, cot) = args
    T, H = shape["tm"], shape["height"]
    Fl, Rl, Cl, CH = latent.shape
    F, R, C, C2 = cot.shape
    N = T * H
    U = H * CH // T
    fits = (
        shape["dp"] % 2 == 0
        and CH % 128 == 0 and U % CH == 0
        and w_b.shape[0] % 16 == 0 and (CH // T) % 16 == 0
        and (9 * C2) % (16 * N) == 0 and C2 % 256 == 0
        and Cl % 16 == 0 and w_l.shape[0] == 27 * U and F >= 2
    )
    if not fits:
        return local(*args)
    sizes = (T, H, Fl, Rl, Cl, CH, C2, F, R, C)
    n_send = 16 + 4 * T + 4 * N + 6 * N + 3 * N
    FL = T * Fl
    band = Rl // H
    cells = F * R * C
    out_rows = 9 * C2 // N
    vmem = pl.BlockSpec(memory_space=pltpu.VMEM)
    flops = 2 * (FL * Rl * Cl * w_l.size + 2 * cells * 27 * C2 * C2 + cells * 9 * C2 * C2)
    outs = pl.pallas_call(
        functools.partial(block_kernel, sizes, n_send),
        out_shape=(
            jax.ShapeDtypeStruct(cot.shape, BF16),
            jax.ShapeDtypeStruct(cot.shape, BF16),
            jax.ShapeDtypeStruct((out_rows, C2), F32),
            jax.ShapeDtypeStruct((8, C2), F32),
        ),
        in_specs=[vmem] * 9,
        out_specs=(vmem,) * 4,
        scratch_shapes=[
            pltpu.VMEM((Fl, Rl, Cl, CH), BF16),
            pltpu.VMEM((T, FL + 2, Rl + 2, Cl, U), BF16),
            pltpu.VMEM((3, FL * Rl * Cl, CH), F32),
            pltpu.VMEM((FL, Rl, Cl, CH), F32),
            pltpu.VMEM((N, Fl, band, Cl, CH), F32),
            pltpu.VMEM((T, 8, CH), F32),
            pltpu.VMEM((N, 8, C2), F32),
            pltpu.VMEM((N, 8, C2), F32),
            pltpu.VMEM((H * CH, 8 * C2), BF16),
            pltpu.VMEM((27 * C2, C2), BF16),
            pltpu.VMEM((cells, C2), F32),
            pltpu.VMEM((cells, C2), F32),
            pltpu.VMEM((F + 2, R + 2, C, C2), BF16),
            pltpu.VMEM((F + 2, R + 2, C, C2), BF16),
            pltpu.VMEM((cells, 3 * C2), BF16),
            pltpu.VMEM((9 * C2, C2), BF16),
            pltpu.VMEM((T, out_rows * H, C2), BF16),
            pltpu.VMEM((out_rows * H, C2), BF16),
            pltpu.VMEM((H, out_rows, C2), BF16),
            pltpu.VMEM((3, cells, C2), F32),
            pltpu.VMEM((C2 // 128, cells, 128), F32),
            pltpu.SemaphoreType.DMA((n_send,)),
            pltpu.SemaphoreType.DMA((n_send,)),
            pltpu.SemaphoreType.DMA((3,)),
        ],
        compiler_params=pltpu.CompilerParams(
            collective_id=0, has_side_effects=True, vmem_limit_bytes=60 * 1024 * 1024
        ),
        cost_estimate=pl.CostEstimate(flops=flops, bytes_accessed=1 << 23, transcendentals=0),
    )(
        latent, gain_l.reshape(1, -1), shift_l.reshape(1, -1), w_l, up_w,
        gain_b.reshape(1, -1), shift_b.reshape(1, -1), w_b, cot,
    )
    decoded, grad_up, grad_w, grad_gs = outs
    return decoded, grad_up, grad_w, grad_gs[0], grad_gs[1]


def solution(mesh):
    return jax.shard_map(
        functools.partial(local_block, dict(mesh.shape)),
        mesh=mesh,
        in_specs=(
            P(("dp", "tm"), None, None, "height"),
            P("height"),
            P("height"),
            P("tm", "height"),
            P("height", None),
            P(),
            P(),
            P(("tm", "height"), None),
            P(("dp", "tm"), "height", None, None),
        ),
        out_specs=(
            P(("dp", "tm"), "height", None, None),
            P(("dp", "tm"), "height", None, None),
            P(("dp", "tm", "height"), None),
            P("dp"),
            P("dp"),
        ),
        check_vma=False,
    )
```
